32 devices in a mesh: seq: 16 (over z, y, core), head: 2 (over x).
Axes of the slice: x: 2, y: 2, z: 4, core: 2. Of those that a mesh axis runs over, the one named last changes fastest.
Arguments:
- queries: bfloat16 [256, 64, 128], P('seq', 'head'), may hold values from -5 to 5
- cache: bfloat16 [2, 1024, 8, 128, 128], P(None, 'seq', 'head'), may hold values from -5 to 5
- page_table: int32 [256, 64], replicated, may hold values from 0 to 1023, as said below
- page_count: int32 [256], replicated, may hold values from 32 to 64, as said below
- out_weight: bfloat16 [8192, 8192], P('head', 'seq'), may hold values from -0.0625 to 0.0625
Outputs:
- output: bfloat16 [256, 8192], P('head', 'seq')
The draws below stay inside these ranges and needn't reach their ends.
Inputs may be any that keep to these rules, and one draw needn't show every extreme that they name: `page_table`: within a row all 64 entries are distinct page ids; only the first page_count entries of a row are selected, the rest are arbitrary. In every row at most 4 entries lie in one aligned block of 64 page ids, and the first 4 entries of every row lie in one such block. `page_count`: some sequence has exactly 64 selected pages.
All inputs are finite; a program needn't handle non-finite values.
Results may differ from the reference program's by a relative error of at most 0.0095.
Values may be sent and summed in bfloat16 or wider, within the bound.
No kernel may reach another device: no remote copies, remote signals or barrier semaphores. Data moves between devices by JAX's collectives and lax.ppermute only.
A program may use at most 192 MiB of HBM per device.

```python
import math
import jax
import jax.numpy as jnp
from jax import lax

D = 8192
QH = 64
KVH = 8
HD = 128
PAGE = 128
SEL = 64
CAP = 4
PAGES_DEV = 64
BATCH = 256
POOL = 1024


def draw_queries(key, part):
    values = jnp.clip(jax.random.normal(jax.random.fold_in(key, 1), (BATCH, QH, HD), jnp.float32), -5.0, 5.0)
    return values.astype(jnp.bfloat16)


def draw_cache(key, part):
    values = jnp.clip(jax.random.normal(jax.random.fold_in(key, 2), (2, POOL, KVH, PAGE, HD), jnp.float32), -5.0, 5.0)
    return values.astype(jnp.bfloat16)


def table_row(stream):
    blocks = POOL // PAGES_DEV
    first_block = jax.random.randint(jax.random.fold_in(stream, 1), (), 0, blocks)
    shuffled = jax.random.permutation(jax.random.fold_in(stream, 2), (blocks - 1) * CAP)
    others = (shuffled // CAP + first_block + 1) % blocks
    block_of = jnp.concatenate([jnp.full((CAP,), first_block, jnp.int32), others[:SEL - CAP].astype(jnp.int32)])
    position = jnp.arange(SEL, dtype=jnp.int32)
    earlier = (block_of[None, :] == block_of[:, None]) & (position[None, :] < position[:, None])
    rank = jnp.sum(earlier.astype(jnp.int32), axis=1)
    within = jax.random.permutation(jax.random.fold_in(stream, 3), PAGES_DEV).astype(jnp.int32)
    return block_of * PAGES_DEV + within[rank]


def draw_page_table(key, part):
    streams = jax.random.split(jax.random.fold_in(key, 21), BATCH)
    return jax.vmap(table_row)(streams).astype(jnp.int32)


def draw_page_count(key, part):
    counts = jax.random.randint(jax.random.fold_in(key, 22), (BATCH,), SEL // 2, SEL + 1)
    fullest = jax.random.randint(jax.random.fold_in(key, 23), (), 0, BATCH)
    return jnp.where(jnp.arange(BATCH, dtype=jnp.int32) == fullest, SEL, counts).astype(jnp.int32)


def levels(rng, dims, cuts, smallest, high):
    loudness = 1.0
    for axis_at, blocks in cuts:
        heights = jax.random.uniform(jax.random.fold_in(jax.random.fold_in(rng, 6), axis_at), (blocks,), jnp.float32, smallest / len(cuts), high / len(cuts))
        loudness = loudness * jnp.repeat(jnp.exp(heights), dims[axis_at] // blocks).reshape((-1,) + (1,) * (len(dims) - 1 - axis_at))
    return loudness


def normal_values(key, extent, width, bound, shards=(), kind=jnp.bfloat16):
    values = jax.random.normal(key, extent, jnp.float32) * width
    if len(shards) > 0:
        values = levels(key, extent, shards, -0.22, 0.18) * values
    return jnp.clip(values, min=-bound, max=bound).astype(kind)


def setup_inputs(seed: int = 0) -> dict:
    arg_keys = jax.random.split(jax.random.key(seed), 6)
    return {
        "queries": draw_queries(jax.random.fold_in(arg_keys[5], 71), 0),
        "cache": draw_cache(jax.random.fold_in(arg_keys[5], 71), 0),
        "page_table": draw_page_table(jax.random.fold_in(arg_keys[5], 71), 0),
        "page_count": draw_page_count(jax.random.fold_in(arg_keys[5], 71), 0),
        "out_weight": normal_values(arg_keys[4], (QH * HD, D), (QH * HD) ** -0.5, 0.0625, ((0, 2), (1, 16))),
    }


def reference(queries, cache, page_table, page_count, out_weight):
    group_size = QH // KVH
    score_scale = 1.0 / math.sqrt(HD)

    def attend_sequence(inputs):
        query, selected, counts = inputs
        key_pages = cache[0][selected].astype(jnp.float32)
        value_pages = cache[1][selected].astype(jnp.float32)
        grouped = query.reshape(KVH, group_size, HD).astype(jnp.float32)
        scores = jnp.einsum('kgd,pktd->kgpt', grouped, key_pages) * score_scale
        usable = (jnp.arange(SEL, dtype=jnp.int32) < counts)[None, None, :, None]
        scores = jnp.where(usable, scores, jnp.float32(-1e+30))
        largest = lax.optimization_barrier(jnp.max(scores, axis=(2, 3), keepdims=True))
        weights = jnp.where(usable, jnp.exp(scores - largest), jnp.float32(0.0))
        totals = lax.optimization_barrier(jnp.sum(weights, axis=(2, 3)))
        rounded = lax.optimization_barrier(weights.astype(jnp.bfloat16)).astype(jnp.float32)
        outputs = jnp.einsum('kgpt,pktd->kgd', rounded, value_pages)
        return (outputs / totals[:, :, None]).reshape(QH * HD).astype(jnp.bfloat16)
    attention = lax.map(attend_sequence, (queries, page_table, page_count))
    return jnp.dot(attention, out_weight, preferred_element_type=jnp.float32).astype(jnp.bfloat16)
```

```python
import functools
import math

import jax
import jax.numpy as jnp
from jax import lax
from jax.experimental import pallas as pl
from jax.experimental.pallas import tpu as pltpu
from jax.sharding import PartitionSpec as P

CAP = 4
TILE = 16
LEAD = 2
NONE = -1e30
PLANES = 3
LANES = 128


def call(body, out_shape, in_specs, out_specs, flops, moved, **kw):
    return pl.pallas_call(
        body,
        out_shape=out_shape,
        in_specs=in_specs,
        out_specs=out_specs,
        cost_estimate=pl.CostEstimate(flops=flops, bytes_accessed=moved, transcendentals=0),
        **kw,
    )


SMEM = pl.BlockSpec(memory_space=pltpu.SMEM)
VMEM = pl.BlockSpec(memory_space=pltpu.VMEM)
ANY = pl.BlockSpec(memory_space=pl.ANY)


def list_kernel(pages, pairs, idx_ref, lst_ref, gp_ref, ng_ref, cnt, base):
    @pl.loop(0, pages + 1)
    def _(p):
        cnt[p] = 0

    slots = lst_ref.shape[0]

    @pl.loop(0, slots // 8)
    def _(i):
        for u in range(8):
            lst_ref[i * 8 + u] = pairs

    @pl.loop(0, gp_ref.shape[0])
    def _(i):
        gp_ref[i] = 0

    @pl.loop(0, pairs // 4)
    def _(i):
        for u in range(4):
            p = idx_ref[i * 4 + u]
            cnt[p] = cnt[p] + 1

    def place(p, g):
        base[p] = g * TILE
        n = (cnt[p] + (TILE - 1)) // TILE

        def mark(i, c):
            gp_ref[g + i] = p
            return c

        lax.fori_loop(0, n, mark, 0)
        return g + n

    end = lax.fori_loop(0, pages, place, LEAD)
    ng_ref[0] = end - LEAD
    base[pages] = slots - 1

    @pl.loop(0, pairs // 4)
    def _(i):
        for u in range(4):
            t = i * 4 + u
            p = idx_ref[t]
            d = base[p]
            real = p < pages
            lst_ref[d] = jnp.where(real, t, pairs)
            base[p] = jnp.where(real, d + 1, d)


def split3(x):
    parts = []
    for _ in range(PLANES):
        part = x.astype(jnp.bfloat16)
        parts.append(part)
        x = x - part.astype(jnp.float32)
    return jnp.concatenate(parts, axis=0)


def join3(block, heads):
    x = block.astype(jnp.float32)
    return (x[:heads] + x[heads : 2 * heads]) + x[2 * heads :]


def attention_kernel(nq, kv, group, scale, lst, gp, ng, valid, *refs):
    q_refs = refs[:nq]
    cache = refs[nq]
    outs = refs[nq + 1 : 2 * nq + 1]
    rest = refs[2 * nq + 1 :]
    kbuf, vbuf, ksem, vsem = rest[:4]
    rest = rest[4:]
    q32, osc, lsc, ssc, psc = (rest[i * kv : (i + 1) * kv] for i in range(5))
    per = q_refs[0].shape[0]
    heads = kv * group
    kcopy = pltpu.make_async_copy(cache.at[0], kbuf, ksem)
    vcopy = pltpu.make_async_copy(cache.at[1], vbuf, vsem)
    kcopy.start()
    vcopy.start()
    for a in range(nq):

        @pl.loop(0, per)
        def _(s):
            row = q_refs[a][s].astype(jnp.float32)
            for k in range(kv):
                q32[k][a * per + s] = row[k * group : (k + 1) * group]

    kcopy.wait()
    vcopy.wait()

    @pl.loop(0, ng[0] + LEAD)
    def _(i):
        t3 = [lst[i * TILE + u] for u in range(TILE)]
        t2 = [lst[(i + 1) * TILE + u] for u in range(TILE)]
        t1 = [lst[(i + 2) * TILE + u] // CAP for u in range(TILE)]
        p3 = gp[i]
        p1 = gp[i + 2]
        for k in range(kv):
            o = jnp.dot(psc[k][...], vbuf[p3, k], preferred_element_type=jnp.float32)
            for u in range(TILE):
                osc[k][t3[u]] = o[u * group : (u + 1) * group]
        for k in range(kv):
            s = ssc[k][...]
            m = jnp.max(s, axis=1, keepdims=True)
            w = jnp.exp2(s - m)
            total = jnp.sum(w, axis=1, keepdims=True)
            psc[k][...] = (w * (1.0 / total)).astype(jnp.bfloat16)
            lse = jnp.broadcast_to(m + jnp.log2(total), s.shape)
            for u in range(TILE):
                lsc[k][t2[u]] = lse[u * group : (u + 1) * group]
        for k in range(kv):
            rows = jnp.concatenate([q32[k][t1[u]] for u in range(TILE)], axis=0)
            s = lax.dot_general(
                rows.astype(jnp.bfloat16),
                kbuf[p1, k],
                (((1,), (1,)), ((), ())),
                preferred_element_type=jnp.float32,
            )
            ssc[k][...] = s * scale

    lane = lax.broadcasted_iota(jnp.int32, (heads, LANES), 1)
    for a in range(nq):

        def finish(s, stats):
            b = a * per + s
            n = valid[b]
            os, ls = [], []
            for k in range(kv):
                l = [jnp.where(n > r, lsc[k][b * CAP + r], NONE) for r in range(CAP)]
                o = [jnp.where(n > r, osc[k][b * CAP + r], 0.0) for r in range(CAP)]
                top = functools.reduce(jnp.maximum, l)
                w = [jnp.exp2(x - top) for x in l]
                total = sum(w[1:], w[0])
                acc = w[0] * o[0]
                for r in range(1, CAP):
                    acc = acc + w[r] * o[r]
                os.append(acc * (1.0 / total))
                ls.append(top + jnp.log2(total))
            outs[a][pl.ds(pl.multiple_of(s * heads, heads), heads), :] = jnp.concatenate(os, axis=0).astype(jnp.bfloat16)
            return jnp.where(lane == s, jnp.concatenate(ls, axis=0), stats)

        stats = lax.fori_loop(0, per, finish, jnp.full((heads, LANES), NONE, jnp.float32))
        outs[a][per * heads :, :] = split3(stats)


def merge_kernel(per, heads, keep, recv, *outs):
    rows = per * heads
    la = join3(keep[rows:, :], heads)
    lb = join3(recv[rows:, :], heads)
    diff = la - lb
    weight = 1.0 / (1.0 + jnp.exp2(-diff))
    each = per // len(outs)
    for s in range(per):
        sl = slice(s * heads, (s + 1) * heads)
        x = keep[sl, :].astype(jnp.float32)
        y = recv[sl, :].astype(jnp.float32)
        z = y + weight[:, s : s + 1] * (x - y)
        at = s % each
        outs[s // each][at * heads : (at + 1) * heads, :] = z.astype(jnp.bfloat16)
    if len(outs) > 1:
        stats = jnp.maximum(la, lb) + jnp.log2(1.0 + jnp.exp2(-jnp.abs(diff)))
        for i, out in enumerate(outs):
            part = stats if i == 0 else jnp.concatenate([stats[:, i * each :], stats[:, : i * each]], axis=1)
            out[each * heads :, :] = split3(part)


def merge(keep, recv, per, heads, last):
    if last:
        shapes = [jax.ShapeDtypeStruct((per * heads, LANES), jnp.bfloat16)]
    else:
        shapes = [jax.ShapeDtypeStruct(((per // 2 + PLANES) * heads, LANES), jnp.bfloat16)] * 2
    return call(
        functools.partial(merge_kernel, per, heads),
        shapes,
        [VMEM] * 2,
        [VMEM] * len(shapes),
        keep.size * 8,
        keep.size * 6,
        name="merge",
        compiler_params=pltpu.CompilerParams(vmem_limit_bytes=8 * 2**20),
    )(keep, recv)


def shards(n, nh, queries, cache, page_table, page_count, out_weight):
    me = lax.axis_index("seq")
    my_head = lax.axis_index("head")
    _, pages, kv, page_len, head_dim = cache.shape
    local, heads, _ = queries.shape
    group = heads // kv
    batch, slots = page_table.shape
    bits = [1 << i for i in range(n.bit_length() - 1)]
    outer = bits[1:]
    halves = 2
    half = local // halves
    orders = [outer, outer[1::-1] + outer[2:]]

    def swap(x, bit):
        return lax.ppermute(x, "seq", [(i, i ^ bit) for i in range(n)])

    per = half * n // 2
    rel = []
    for a in range(halves):
        for c in range(2):
            for s in range(n // 2):
                j = c * bits[0]
                for at, bit in enumerate(orders[a]):
                    if (s >> (len(outer) - 1 - at)) & 1:
                        j |= bit
                rel.append((j, a))
    rel_j = jnp.array([j for j, _ in rel], jnp.int32)
    rel_a = jnp.array([a for _, a in rel], jnp.int32)
    true_block = (rel_j ^ me) * halves + rel_a

    table = page_table.reshape(-1, half, slots)[true_block].reshape(batch, slots)
    counts = page_count.reshape(-1, half)[true_block].reshape(batch)
    position = jnp.arange(slots, dtype=jnp.int32)
    present = (position[None, :] < counts[:, None]) & (table // pages == me)
    upper = (position[:, None] <= position[None, :]).astype(jnp.float32)
    ranks = jnp.dot(present.astype(jnp.float32), upper).astype(jnp.int32) - 1
    onehot = present[:, None, :] & (ranks[:, None, :] == jnp.arange(CAP, dtype=jnp.int32)[None, :, None])
    valid = jnp.sum(present.astype(jnp.int32), axis=1)
    index = jnp.sum(jnp.where(onehot, table[:, None, :] - me * pages, 0), axis=2)
    index = jnp.where(jnp.arange(CAP)[None, :] < valid[:, None], index, pages).reshape(-1)

    pairs = batch * CAP
    most = pages + pairs // TILE + 2 * LEAD
    lst, gp, ng = call(
        functools.partial(list_kernel, pages, pairs),
        [jax.ShapeDtypeStruct((s,), jnp.int32) for s in (most * TILE, most, 1)],
        [SMEM],
        [SMEM] * 3,
        10**9,
        10**6,
        scratch_shapes=[pltpu.SMEM((pages + 1,), jnp.int32)] * 2,
        name="lists",
        compiler_params=pltpu.CompilerParams(vmem_limit_bytes=2**20),
    )(index)

    got = [queries[a * half : (a + 1) * half] for a in range(halves)]
    for at in reversed(range(len(outer))):
        new = [swap(x, orders[a][at]) for a, x in enumerate(got)]
        got = [jnp.concatenate([x, y], axis=0) for x, y in zip(got, new)]
    q_parts = []
    for x in got:
        q_parts += [x, swap(x, bits[0])]

    nq = 2 * halves
    tile = (pairs + 1, group, head_dim)
    scratch = [pltpu.VMEM(cache.shape[1:], cache.dtype)] * 2 + [pltpu.SemaphoreType.DMA] * 2
    scratch += [pltpu.VMEM((batch + 1, group, head_dim), jnp.float32)] * kv
    scratch += [pltpu.VMEM(tile, jnp.float32)] * (2 * kv)
    scratch += [pltpu.VMEM((TILE * group, page_len), jnp.float32)] * kv
    scratch += [pltpu.VMEM((TILE * group, page_len), jnp.bfloat16)] * kv
    parts = call(
        functools.partial(attention_kernel, nq, kv, group, math.log2(math.e) / math.sqrt(head_dim)),
        [jax.ShapeDtypeStruct(((per + PLANES) * heads, LANES), jnp.bfloat16)] * nq,
        [SMEM] * 4 + [VMEM] * nq + [ANY],
        [VMEM] * nq,
        4 * pairs * heads * page_len * head_dim,
        cache.size * 2,
        scratch_shapes=scratch,
        name="attention",
        compiler_params=pltpu.CompilerParams(vmem_limit_bytes=63 * 2**20),
    )(lst, gp, ng, valid, *q_parts, cache)

    keep = [parts[2 * a] for a in range(halves)]
    send = [parts[2 * a + 1] for a in range(halves)]
    now = per
    att = [None] * halves
    for at in range(len(bits)):
        took = [swap(send[a], ([bits[0]] + orders[a])[at]) for a in range(halves)]
        for a in range(halves):
            last = at == len(bits) - 1
            res = merge(keep[a], took[a], now, heads, last)
            if last:
                att[a] = res[0].reshape(half, heads * head_dim)
            else:
                keep[a], send[a] = res
        now //= 2

    for at in reversed(range(len(outer))):
        new = [swap(x, orders[a][at]) for a, x in enumerate(att)]
        att = [jnp.concatenate([x, y], axis=0) for x, y in zip(att, new)]
    rows = []
    for x in att:
        rows += [x, swap(x, bits[0])]
    product = jnp.dot(jnp.concatenate(rows, axis=0), out_weight, preferred_element_type=jnp.float32)

    width = product.shape[1]
    place = {ja: i for i, ja in enumerate(rel)}
    inverse = jnp.array([place[(j, a)] for j in range(n) for a in range(halves)], jnp.int32).reshape(n, halves)
    source = inverse[jnp.arange(n, dtype=jnp.int32) ^ me].reshape(nh, -1)
    blocks = product.reshape(n * halves, half, width)
    out = blocks[source[my_head]].reshape(batch // nh, width)
    for step in range(1, nh):
        give = blocks[source[my_head ^ step]].astype(jnp.bfloat16).reshape(batch // nh, width)
        took = lax.ppermute(give, "head", [(i, i ^ step) for i in range(nh)])
        out = out + took.astype(jnp.float32)
    return out.astype(jnp.bfloat16)


def solution(mesh):
    n, nh = mesh.shape["seq"], mesh.shape["head"]
    return jax.shard_map(
        functools.partial(shards, n, nh),
        mesh=mesh,
        in_specs=(
            P("seq", "head", None),
            P(None, "seq", "head", None, None),
            P(),
            P(),
            P("head", "seq"),
        ),
        out_specs=P("head", "seq"),
        check_vma=False,
    )
```

```python
import functools
import math

import jax
import jax.numpy as jnp
from jax import lax
from jax.experimental import pallas as pl
from jax.experimental.pallas import tpu as pltpu
from jax.sharding import PartitionSpec as P

CAP = 4
TILE = 16
SEGMENTS = 4
TOGETHER = 2
UNROLL = 4
LEAD = 2 * TOGETHER
NONE = -1e30
PLANES = 3
LANES = 128


def call(body, out_shape, in_specs, out_specs, flops, moved, **kw):
    return pl.pallas_call(
        body,
        out_shape=out_shape,
        in_specs=in_specs,
        out_specs=out_specs,
        cost_estimate=pl.CostEstimate(flops=flops, bytes_accessed=moved, transcendentals=0),
        **kw,
    )


SMEM = pl.BlockSpec(memory_space=pltpu.SMEM)
VMEM = pl.BlockSpec(memory_space=pltpu.VMEM)
ANY = pl.BlockSpec(memory_space=pl.ANY)


def list_kernel(pages, me_ref, table_ref, count_ref, lst_ref, gp_ref, start_ref, valid_ref):
    batch, slots = table_ref.shape
    most = gp_ref.shape[1]
    f32, bf16, i32 = jnp.float32, jnp.bfloat16, jnp.int32

    def iota(shape, axis):
        return lax.broadcasted_iota(i32, shape, axis)

    def ones_where(mask):
        return jnp.where(mask, 1.0, 0.0).astype(bf16)

    def dot(x, y, dims=((1,), (0,)), **kw):
        return lax.dot_general(x, y, (dims, ((), ())), preferred_element_type=f32, **kw)

    page = table_ref[...] - me_ref[0] * pages
    present = (iota((batch, slots), 1) < count_ref[...]) & (page >= 0) & (page < pages)
    here = ones_where(present)
    upto = dot(here, ones_where(iota((slots, slots), 0) <= iota((slots, slots), 1)))
    valid_ref[...] = dot(jnp.ones((8, slots), bf16), here, ((1,), (1,)))[:1].astype(i32)
    hot = []
    for r in range(CAP):
        mine = present & (upto == r + 1.0)
        chosen = jnp.max(jnp.where(mine, page, -1), axis=1, keepdims=True)
        hot.append(jnp.where(iota((batch, pages), 1) == chosen, 1.0, 0.0))
    every = sum(hot[1:], hot[0]).astype(bf16)
    before = dot(ones_where(iota((batch, batch), 0) > iota((batch, batch), 1)), every)

    def groups(n):
        return jnp.floor((n + (TILE - 1.0)) * (1.0 / TILE))

    exact = dict(precision=lax.Precision.HIGHEST)
    row = groups(dot(jnp.ones((8, batch), bf16), every))
    under = jnp.where(iota((pages, pages), 0) < iota((pages, pages), 1), 1.0, 0.0)
    base = dot(row, under, **exact)[:1] + LEAD
    place = base * TILE + before
    col = groups(dot(every, jnp.ones((batch, LANES), bf16), ((0,), (0,))))
    over = jnp.where(iota((pages, pages), 1) < iota((pages, pages), 0), 1.0, 0.0)
    base_col = dot(over, col, **exact)[:, :1] + LEAD
    at_most = jnp.where(base_col <= iota((pages, most), 1).astype(f32), 1.0, 0.0)
    gp_ref[...] = jnp.maximum(jnp.sum(at_most, axis=0, keepdims=True) - 1.0, 0.0).astype(i32)

    bound = iota((pages, LANES), 1) * (pages // SEGMENTS)
    start_ref[...] = jnp.sum(jnp.where(iota((pages, LANES), 0) < bound, col, 0.0), axis=0, keepdims=True).astype(i32)

    size = lst_ref.shape[1]
    total = jnp.zeros((8, size), f32)
    for r in range(CAP):
        to = jnp.sum(jnp.where(hot[r] > 0.0, place + 1.0, 0.0), axis=1, keepdims=True).astype(i32) - 1
        onto = ones_where(iota((batch, size), 1) == to)
        pair = iota((8, batch), 1) * CAP + r
        which = iota((8, batch), 0)
        parts = jnp.where(which == 0, pair // 64, jnp.where(which == 1, pair % 64, 1)).astype(f32)
        total = total + dot(parts.astype(bf16), onto)
    found = total[0:1] * 64.0 + total[1:2]
    lst_ref[...] = jnp.where(total[2:3] > 0.5, found, float(batch * CAP)).astype(i32)


def make_lists(me, table, counts, pages):
    batch, slots = table.shape
    most = -(-(pages + batch * CAP // TILE + 2 * LEAD + TOGETHER) // 8) * 8
    shapes = [(1, most * TILE), (1, most), (1, LANES), (1, batch)]
    return call(
        functools.partial(list_kernel, pages),
        [jax.ShapeDtypeStruct(s, jnp.int32) for s in shapes],
        [SMEM, VMEM, VMEM],
        [VMEM] * 4,
        10**8,
        10**6,
        name="lists",
        compiler_params=pltpu.CompilerParams(vmem_limit_bytes=16 * 2**20),
    )(me.reshape(1), table, counts.reshape(batch, 1))


def split3(x):
    parts = []
    for _ in range(PLANES):
        part = x.astype(jnp.bfloat16)
        parts.append(part)
        x = x - part.astype(jnp.float32)
    return jnp.concatenate(parts, axis=0)


def join3(block, heads):
    x = block.astype(jnp.float32)
    return (x[:heads] + x[heads : 2 * heads]) + x[2 * heads :]


def attention_kernel(nq, kv, group, scale, lst, gp, start, valid, *refs):
    q_refs = refs[:nq]
    cache = refs[nq]
    outs = refs[nq + 1 : 2 * nq + 1]
    kbuf, vbuf, sems, q32, osc, lsc, ssc, msc, psc = refs[2 * nq + 1 :]
    per = q_refs[0].shape[0]
    heads = kv * group
    pairs = nq * per * CAP
    head_dim = vbuf.shape[-1]
    chunk = kbuf.shape[0] // SEGMENTS
    ones = jnp.ones(vbuf.shape[-2:-1] + (LANES,), jnp.bfloat16)

    def copies(g):
        at = pl.ds(g * chunk, chunk)
        return (
            pltpu.make_async_copy(cache.at[0, at], kbuf.at[at], sems.at[0, g]),
            pltpu.make_async_copy(cache.at[1, at], vbuf.at[at], sems.at[1, g]),
        )

    for g in range(SEGMENTS):
        for c in copies(g):
            c.start()

    def convert(a, i):
        for u in range(8):
            row = q_refs[a][i * 8 + u].astype(jnp.float32)
            q32[a * per + i * 8 + u] = row.reshape(kv, group, head_dim)

    for a in range(nq):
        pl.loop(0, per // 8)(functools.partial(convert, a))
    q32[nq * per] = jnp.zeros((kv, group, head_dim), jnp.float32)
    osc[pairs + 1] = jnp.zeros((heads, head_dim), jnp.bfloat16)
    lsc[pairs + 1] = jnp.full((kv, group, LANES), NONE, jnp.float32)

    def step(j):
        def entries(stage, v):
            i = (j + stage) * TOGETHER + v
            return gp[0, i], [lst[0, i * TILE + u] for u in range(TILE)]

        for v in range(TOGETHER):
            page, t = entries(0, v)
            os = []
            for k in range(kv):
                values = jnp.concatenate([vbuf[page, k], ones], axis=1)
                o = jnp.dot(psc[v, k], values, preferred_element_type=jnp.float32)
                total = o[:, head_dim:]
                os.append(o[:, :head_dim] * (1.0 / total))
                lse = msc[v, k] + jnp.log2(total)
                for u in range(TILE):
                    lsc[t[u], k] = lse[u * group : (u + 1) * group]
            for u in range(TILE):
                tiles = [o[u * group : (u + 1) * group] for o in os]
                osc[t[u]] = jnp.concatenate(tiles, axis=0).astype(jnp.bfloat16)
        for v in range(TOGETHER):
            for k in range(kv):
                s = ssc[v, k]
                m = jnp.broadcast_to(jnp.max(s, axis=1, keepdims=True), s.shape)
                psc[v, k] = jnp.exp2(s - m).astype(jnp.bfloat16)
                msc[v, k] = m
        for v in range(TOGETHER):
            page, t = entries(2, v)
            b = [x // CAP for x in t]
            for k in range(kv):
                rows = jnp.concatenate([q32[x, k] for x in b], axis=0)
                s = lax.dot_general(
                    rows.astype(jnp.bfloat16),
                    kbuf[page, k],
                    (((1,), (1,)), ((), ())),
                    preferred_element_type=jnp.float32,
                )
                ssc[v, k] = s * scale

    for g in range(SEGMENTS):
        for c in copies(g):
            c.wait()
        end = start[0, g + 1]
        if g == SEGMENTS - 1:
            end = end + (3 * TOGETHER - 1)
        pl.loop(start[0, g] // TOGETHER, end // TOGETHER)(step)

    lane = lax.broadcasted_iota(jnp.int32, (heads, LANES), 1)
    for a in range(nq):

        def finish(s, stats):
            b = a * per + s
            n = valid[0, b]
            t = [jnp.where(n > r, b * CAP + r, pairs + 1) for r in range(CAP)]
            l = [lsc[x].reshape(heads, LANES) for x in t]
            top = functools.reduce(jnp.maximum, l)
            w = [jnp.exp2(x - top) for x in l]
            total = sum(w[1:], w[0])
            terms = [x * osc[y].astype(jnp.float32) for x, y in zip(w, t)]
            o = sum(terms[1:], terms[0]) * (1.0 / total)
            outs[a][pl.ds(pl.multiple_of(s * heads, heads), heads), :] = o.astype(jnp.bfloat16)
            return jnp.where(lane == s, top + jnp.log2(total), stats)

        stats = lax.fori_loop(0, per, finish, jnp.full((heads, LANES), NONE, jnp.float32), unroll=UNROLL)
        outs[a][per * heads :, :] = split3(stats)


def merge_kernel(per, heads, keep, recv, *outs):
    rows = per * heads
    la = join3(keep[rows:, :], heads)
    lb = join3(recv[rows:, :], heads)
    diff = la - lb
    weight = 1.0 / (1.0 + jnp.exp2(-diff))
    each = per // len(outs)
    for s in range(per):
        sl = slice(s * heads, (s + 1) * heads)
        x = keep[sl, :].astype(jnp.float32)
        y = recv[sl, :].astype(jnp.float32)
        z = y + weight[:, s : s + 1] * (x - y)
        at = s % each
        outs[s // each][at * heads : (at + 1) * heads, :] = z.astype(jnp.bfloat16)
    if len(outs) > 1:
        stats = jnp.maximum(la, lb) + jnp.log2(1.0 + jnp.exp2(-jnp.abs(diff)))
        for i, out in enumerate(outs):
            part = stats if i == 0 else jnp.concatenate([stats[:, i * each :], stats[:, : i * each]], axis=1)
            out[each * heads :, :] = split3(part)


def merge(keep, recv, per, heads, last):
    if last:
        shapes = [jax.ShapeDtypeStruct((per * heads, LANES), jnp.bfloat16)]
    else:
        shapes = [jax.ShapeDtypeStruct(((per // 2 + PLANES) * heads, LANES), jnp.bfloat16)] * 2
    return call(
        functools.partial(merge_kernel, per, heads),
        shapes,
        [VMEM] * 2,
        [VMEM] * len(shapes),
        keep.size * 8,
        keep.size * 6,
        name="merge",
        compiler_params=pltpu.CompilerParams(vmem_limit_bytes=8 * 2**20),
    )(keep, recv)


def attend(lst, gp, start, valid, q_parts, cache):
    nq = len(q_parts)
    per, heads, head_dim = q_parts[0].shape
    _, pages, kv, page_len, _ = cache.shape
    group = heads // kv
    batch = nq * per
    pairs = batch * CAP
    scratch = [pltpu.VMEM(cache.shape[1:], cache.dtype)] * 2 + [pltpu.SemaphoreType.DMA((2, SEGMENTS))]
    scratch += [pltpu.VMEM((batch + 1, kv, group, head_dim), jnp.float32)]
    scratch += [pltpu.VMEM((pairs + 2, heads, head_dim), jnp.bfloat16)]
    scratch += [pltpu.VMEM((pairs + 2, kv, group, LANES), jnp.float32)]
    scratch += [pltpu.VMEM((TOGETHER, kv, TILE * group, page_len), jnp.float32)] * 2
    scratch += [pltpu.VMEM((TOGETHER, kv, TILE * group, page_len), jnp.bfloat16)]
    return call(
        functools.partial(attention_kernel, nq, kv, group, math.log2(math.e) / math.sqrt(head_dim)),
        [jax.ShapeDtypeStruct(((per + PLANES) * heads, LANES), jnp.bfloat16)] * nq,
        [SMEM] * 4 + [VMEM] * nq + [ANY],
        [VMEM] * nq,
        4 * pairs * heads * page_len * head_dim,
        cache.size * 2,
        scratch_shapes=scratch,
        name="attention",
        compiler_params=pltpu.CompilerParams(vmem_limit_bytes=47 * 2**20),
    )(lst, gp, start, valid, *q_parts, cache)


def shards(n, nh, queries, cache, page_table, page_count, out_weight):
    me = lax.axis_index("seq")
    my_head = lax.axis_index("head")
    _, pages, kv, page_len, head_dim = cache.shape
    local, heads, _ = queries.shape
    group = heads // kv
    batch, slots = page_table.shape
    bits = [1 << i for i in range(n.bit_length() - 1)]
    outer = bits[1:]
    halves = 2
    half = local // halves
    orders = [outer, outer[1::-1] + outer[2:]]

    def swap(x, bit):
        return lax.ppermute(x, "seq", [(i, i ^ bit) for i in range(n)])

    per = half * n // 2
    rel = []
    for a in range(halves):
        for c in range(2):
            for s in range(n // 2):
                j = c * bits[0]
                for at, bit in enumerate(orders[a]):
                    if (s >> (len(outer) - 1 - at)) & 1:
                        j |= bit
                rel.append((j, a))
    rel_j = jnp.array([j for j, _ in rel], jnp.int32)
    rel_a = jnp.array([a for _, a in rel], jnp.int32)
    true_block = (rel_j ^ me) * halves + rel_a

    table = page_table.reshape(-1, half, slots)[true_block].reshape(batch, slots)
    counts = page_count.reshape(-1, half)[true_block].reshape(batch)

    got = [queries[a * half : (a + 1) * half] for a in range(halves)]
    lists = None
    for at in reversed(range(len(outer))):
        new = [swap(x, orders[a][at]) for a, x in enumerate(got)]
        if at == 0:
            lists = make_lists(me, table, counts, pages)
            new, lists = lax.optimization_barrier((new, lists))
        elif at == len(outer) - 1:
            new, table, counts = lax.optimization_barrier((new, table, counts))
        got = [jnp.concatenate([x, y], axis=0) for x, y in zip(got, new)]
    q_parts = []
    for x in got:
        q_parts += [x, swap(x, bits[0])]

    parts = attend(*lists, q_parts, cache)

    keep = [parts[2 * a] for a in range(halves)]
    send = [parts[2 * a + 1] for a in range(halves)]
    now = per
    att = [None] * halves
    for at in range(len(bits)):
        took = [swap(send[a], ([bits[0]] + orders[a])[at]) for a in range(halves)]
        for a in range(halves):
            last = at == len(bits) - 1
            res = merge(keep[a], took[a], now, heads, last)
            if last:
                att[a] = res[0].reshape(half, heads * head_dim)
            else:
                keep[a], send[a] = res
        now //= 2

    for at in reversed(range(len(outer))):
        new = [swap(x, orders[a][at]) for a, x in enumerate(att)]
        att = [jnp.concatenate([x, y], axis=0) for x, y in zip(att, new)]
    rows = []
    for x in att:
        rows += [x, swap(x, bits[0])]
    product = jnp.dot(jnp.concatenate(rows, axis=0), out_weight, preferred_element_type=jnp.float32)

    width = product.shape[1]
    place = {ja: i for i, ja in enumerate(rel)}
    inverse = jnp.array([place[(j, a)] for j in range(n) for a in range(halves)], jnp.int32).reshape(n, halves)
    source = inverse[jnp.arange(n, dtype=jnp.int32) ^ me].reshape(nh, -1)
    blocks = product.reshape(n * halves, half, width)
    out = blocks[source[my_head]].reshape(batch // nh, width)
    for step in range(1, nh):
        give = blocks[source[my_head ^ step]].astype(jnp.bfloat16).reshape(batch // nh, width)
        took = lax.ppermute(give, "head", [(i, i ^ step) for i in range(nh)])
        out = out + took.astype(jnp.float32)
    return out.astype(jnp.bfloat16)


def solution(mesh):
    n, nh = mesh.shape["seq"], mesh.shape["head"]
    return jax.shard_map(
        functools.partial(shards, n, nh),
        mesh=mesh,
        in_specs=(
            P("seq", "head", None),
            P(None, "seq", "head", None, None),
            P(),
            P(),
            P("head", "seq"),
        ),
        out_specs=P("head", "seq"),
        check_vma=False,
    )
```

```python
import functools
import math

import jax
import jax.numpy as jnp
from jax import lax
from jax.experimental import pallas as pl
from jax.experimental.pallas import tpu as pltpu
from jax.sharding import PartitionSpec as P

CAP = 4
TILE = 16
SEGMENTS = 4
TOGETHER = 4
UNROLL = 4
LEAD = 2 * TOGETHER
NONE = -1e30
PLANES = 3
LANES = 128


def call(body, out_shape, in_specs, out_specs, flops, moved, **kw):
    return pl.pallas_call(
        body,
        out_shape=out_shape,
        in_specs=in_specs,
        out_specs=out_specs,
        cost_estimate=pl.CostEstimate(flops=flops, bytes_accessed=moved, transcendentals=0),
        **kw,
    )


SMEM = pl.BlockSpec(memory_space=pltpu.SMEM)
VMEM = pl.BlockSpec(memory_space=pltpu.VMEM)
ANY = pl.BlockSpec(memory_space=pl.ANY)


def list_kernel(pages, me_ref, table_ref, count_ref, lst_ref, gp_ref, start_ref, valid_ref):
    batch, slots = table_ref.shape
    most = gp_ref.shape[1]
    f32, bf16, i32 = jnp.float32, jnp.bfloat16, jnp.int32

    def iota(shape, axis):
        return lax.broadcasted_iota(i32, shape, axis)

    def ones_where(mask):
        return jnp.where(mask, 1.0, 0.0).astype(bf16)

    def dot(x, y, dims=((1,), (0,)), **kw):
        return lax.dot_general(x, y, (dims, ((), ())), preferred_element_type=f32, **kw)

    page = table_ref[...] - me_ref[0] * pages
    present = (iota((batch, slots), 1) < count_ref[...]) & (page >= 0) & (page < pages)
    here = ones_where(present)
    upto = dot(here, ones_where(iota((slots, slots), 0) <= iota((slots, slots), 1)))
    valid_ref[...] = dot(jnp.ones((8, slots), bf16), here, ((1,), (1,)))[:1].astype(i32)
    hot = []
    for r in range(CAP):
        mine = present & (upto == r + 1.0)
        chosen = jnp.max(jnp.where(mine, page, -1), axis=1, keepdims=True)
        hot.append(jnp.where(iota((batch, pages), 1) == chosen, 1.0, 0.0))
    every = sum(hot[1:], hot[0]).astype(bf16)
    before = dot(ones_where(iota((batch, batch), 0) > iota((batch, batch), 1)), every)

    def groups(n):
        return jnp.floor((n + (TILE - 1.0)) * (1.0 / TILE))

    exact = dict(precision=lax.Precision.HIGHEST)
    row = groups(dot(jnp.ones((8, batch), bf16), every))
    under = jnp.where(iota((pages, pages), 0) < iota((pages, pages), 1), 1.0, 0.0)
    base = dot(row, under, **exact)[:1] + LEAD
    place = base * TILE + before
    col = groups(dot(every, jnp.ones((batch, LANES), bf16), ((0,), (0,))))
    over = jnp.where(iota((pages, pages), 1) < iota((pages, pages), 0), 1.0, 0.0)
    base_col = dot(over, col, **exact)[:, :1] + LEAD
    at_most = jnp.where(base_col <= iota((pages, most), 1).astype(f32), 1.0, 0.0)
    gp_ref[...] = jnp.maximum(jnp.sum(at_most, axis=0, keepdims=True) - 1.0, 0.0).astype(i32)

    bound = iota((pages, LANES), 1) * (pages // SEGMENTS)
    start_ref[...] = jnp.sum(jnp.where(iota((pages, LANES), 0) < bound, col, 0.0), axis=0, keepdims=True).astype(i32)

    size = lst_ref.shape[1]
    total = jnp.zeros((8, size), f32)
    for r in range(CAP):
        to = jnp.sum(jnp.where(hot[r] > 0.0, place + 1.0, 0.0), axis=1, keepdims=True).astype(i32) - 1
        onto = ones_where(iota((batch, size), 1) == to)
        pair = iota((8, batch), 1) * CAP + r
        which = iota((8, batch), 0)
        parts = jnp.where(which == 0, pair // 64, jnp.where(which == 1, pair % 64, 1)).astype(f32)
        total = total + dot(parts.astype(bf16), onto)
    found = total[0:1] * 64.0 + total[1:2]
    lst_ref[...] = jnp.where(total[2:3] > 0.5, found, float(batch * CAP)).astype(i32)


def make_lists(me, table, counts, pages):
    batch, slots = table.shape
    most = -(-(pages + batch * CAP // TILE + 2 * LEAD + TOGETHER) // 8) * 8
    shapes = [(1, most * TILE), (1, most), (1, LANES), (1, batch)]
    return call(
        functools.partial(list_kernel, pages),
        [jax.ShapeDtypeStruct(s, jnp.int32) for s in shapes],
        [SMEM, VMEM, VMEM],
        [VMEM] * 4,
        10**8,
        10**6,
        name="lists",
        compiler_params=pltpu.CompilerParams(vmem_limit_bytes=16 * 2**20),
    )(me.reshape(1), table, counts.reshape(batch, 1))


def stat_rows(count, heads):
    return heads if PLANES * count <= LANES else PLANES * heads


def split3(x, count):
    parts = []
    for _ in range(PLANES):
        part = x.astype(jnp.bfloat16).astype(jnp.float32)
        parts.append(part)
        x = x - part
    if PLANES * count > LANES:
        x = jnp.concatenate(parts, axis=0)
        if x.shape[1] < LANES:
            x = jnp.concatenate([x, jnp.zeros((x.shape[0], LANES - x.shape[1]), jnp.float32)], axis=1)
        return x.astype(jnp.bfloat16)
    parts = [p[:, :count] for p in parts]
    rest = LANES - PLANES * count
    if rest:
        parts.append(jnp.zeros((x.shape[0], rest), jnp.float32))
    return jnp.concatenate(parts, axis=1).astype(jnp.bfloat16)


def join3(block, count, heads):
    x = block.astype(jnp.float32)
    if PLANES * count > LANES:
        parts = [x[p * heads : (p + 1) * heads, :count] for p in range(PLANES)]
    else:
        parts = [x[:, p * count : (p + 1) * count] for p in range(PLANES)]
    return (parts[0] + parts[1]) + parts[2]


def attention_kernel(nq, kv, group, scale, lst, gp, start, valid, *refs):
    q_refs = refs[:nq]
    cache = refs[nq]
    outs = refs[nq + 1 : 2 * nq + 1]
    kbuf, vbuf, sems, q32, osc, lsc, ssc, msc, psc = refs[2 * nq + 1 :]
    per = q_refs[0].shape[0]
    heads = kv * group
    pairs = nq * per * CAP
    head_dim = vbuf.shape[-1]
    chunk = kbuf.shape[0] // SEGMENTS
    ones = jnp.ones(vbuf.shape[-2:-1] + (LANES,), jnp.bfloat16)

    def copies(g):
        at = pl.ds(g * chunk, chunk)
        return (
            pltpu.make_async_copy(cache.at[0, at], kbuf.at[at], sems.at[0, g]),
            pltpu.make_async_copy(cache.at[1, at], vbuf.at[at], sems.at[1, g]),
        )

    for c in copies(0):
        c.start()

    def convert(a, i):
        for u in range(8):
            row = q_refs[a][i * 8 + u].astype(jnp.float32)
            q32[a * per + i * 8 + u] = row.reshape(kv, group, head_dim)

    for a in range(nq):
        pl.loop(0, per // 8)(functools.partial(convert, a))
    q32[nq * per] = jnp.zeros((kv, group, head_dim), jnp.float32)
    osc[pairs + 1] = jnp.zeros((heads, head_dim), jnp.bfloat16)
    lsc[pairs + 1] = jnp.full((kv, group, LANES), NONE, jnp.float32)

    def step(j):
        def entries(stage, v):
            i = (j + stage) * TOGETHER + v
            return gp[0, i], [lst[0, i * TILE + u] for u in range(TILE)]

        for v in range(TOGETHER):
            page, t = entries(0, v)
            os = []
            for k in range(kv):
                values = jnp.concatenate([vbuf[page, k], ones], axis=1)
                o = jnp.dot(psc[v, k], values, preferred_element_type=jnp.float32)
                total = o[:, head_dim:]
                os.append(o[:, :head_dim] * (1.0 / total))
                lse = msc[v, k] + jnp.log2(total)
                for u in range(TILE):
                    lsc[t[u], k] = lse[u * group : (u + 1) * group]
            for u in range(TILE):
                tiles = [o[u * group : (u + 1) * group] for o in os]
                osc[t[u]] = jnp.concatenate(tiles, axis=0).astype(jnp.bfloat16)
        for v in range(TOGETHER):
            for k in range(kv):
                s = ssc[v, k]
                m = jnp.broadcast_to(jnp.max(s, axis=1, keepdims=True), s.shape)
                psc[v, k] = jnp.exp2(s - m).astype(jnp.bfloat16)
                msc[v, k] = m
        for v in range(TOGETHER):
            page, t = entries(2, v)
            b = [x // CAP for x in t]
            for k in range(kv):
                rows = jnp.concatenate([q32[x, k] for x in b], axis=0)
                s = lax.dot_general(
                    rows.astype(jnp.bfloat16),
                    kbuf[page, k],
                    (((1,), (1,)), ((), ())),
                    preferred_element_type=jnp.float32,
                )
                ssc[v, k] = s * scale

    for g in range(SEGMENTS):
        for c in copies(g):
            c.wait()
        if g + 1 < SEGMENTS:
            for c in copies(g + 1):
                c.start()
        end = start[0, g + 1]
        if g == SEGMENTS - 1:
            end = end + (3 * TOGETHER - 1)
        pl.loop(start[0, g] // TOGETHER, end // TOGETHER)(step)

    lane = lax.broadcasted_iota(jnp.int32, (heads, LANES), 1)
    for a in range(nq):

        def finish(s, stats):
            b = a * per + s
            n = valid[0, b]
            t = [jnp.where(n > r, b * CAP + r, pairs + 1) for r in range(CAP)]
            l = [lsc[x].reshape(heads, LANES) for x in t]
            top = functools.reduce(jnp.maximum, l)
            w = [jnp.exp2(x - top) for x in l]
            total = sum(w[1:], w[0])
            terms = [x * osc[y].astype(jnp.float32) for x, y in zip(w, t)]
            o = sum(terms[1:], terms[0]) * (1.0 / total)
            outs[a][pl.ds(pl.multiple_of(s * heads, heads), heads), :] = o.astype(jnp.bfloat16)
            return jnp.where(lane == s, top + jnp.log2(total), stats)

        stats = lax.fori_loop(0, per, finish, jnp.full((heads, LANES), NONE, jnp.float32), unroll=UNROLL)
        outs[a][per * heads :, :] = split3(stats, per)


def merge_kernel(per, heads, keep, recv, *outs):
    rows = per * heads
    la = join3(keep[rows:, :], per, heads)
    lb = join3(recv[rows:, :], per, heads)
    diff = la - lb
    weight = 1.0 / (1.0 + jnp.exp2(-diff))
    each = per // len(outs)
    for s in range(per):
        sl = slice(s * heads, (s + 1) * heads)
        x = keep[sl, :].astype(jnp.float32)
        y = recv[sl, :].astype(jnp.float32)
        z = y + weight[:, s : s + 1] * (x - y)
        at = s % each
        outs[s // each][at * heads : (at + 1) * heads, :] = z.astype(jnp.bfloat16)
    if len(outs) > 1:
        stats = jnp.maximum(la, lb) + jnp.log2(1.0 + jnp.exp2(-jnp.abs(diff)))
        for i, out in enumerate(outs):
            out[each * heads :, :] = split3(stats[:, i * each : (i + 1) * each], each)


def merge(keep, recv, per, heads, last):
    if last:
        shapes = [jax.ShapeDtypeStruct((per * heads, LANES), jnp.bfloat16)]
    else:
        shapes = [jax.ShapeDtypeStruct((per // 2 * heads + stat_rows(per // 2, heads), LANES), jnp.bfloat16)] * 2
    return call(
        functools.partial(merge_kernel, per, heads),
        shapes,
        [VMEM] * 2,
        [VMEM] * len(shapes),
        keep.size * 8,
        keep.size * 6,
        name="merge",
        compiler_params=pltpu.CompilerParams(vmem_limit_bytes=8 * 2**20),
    )(keep, recv)


def attend(lst, gp, start, valid, q_parts, cache):
    nq = len(q_parts)
    per, heads, head_dim = q_parts[0].shape
    _, pages, kv, page_len, _ = cache.shape
    group = heads // kv
    batch = nq * per
    pairs = batch * CAP
    scratch = [pltpu.VMEM(cache.shape[1:], cache.dtype)] * 2 + [pltpu.SemaphoreType.DMA((2, SEGMENTS))]
    scratch += [pltpu.VMEM((batch + 1, kv, group, head_dim), jnp.float32)]
    scratch += [pltpu.VMEM((pairs + 2, heads, head_dim), jnp.bfloat16)]
    scratch += [pltpu.VMEM((pairs + 2, kv, group, LANES), jnp.float32)]
    scratch += [pltpu.VMEM((TOGETHER, kv, TILE * group, page_len), jnp.float32)] * 2
    scratch += [pltpu.VMEM((TOGETHER, kv, TILE * group, page_len), jnp.bfloat16)]
    return call(
        functools.partial(attention_kernel, nq, kv, group, math.log2(math.e) / math.sqrt(head_dim)),
        [jax.ShapeDtypeStruct((per * heads + stat_rows(per, heads), LANES), jnp.bfloat16)] * nq,
        [SMEM] * 4 + [VMEM] * nq + [ANY],
        [VMEM] * nq,
        4 * pairs * heads * page_len * head_dim,
        cache.size * 2,
        scratch_shapes=scratch,
        name="attention",
        compiler_params=pltpu.CompilerParams(vmem_limit_bytes=47 * 2**20),
    )(lst, gp, start, valid, *q_parts, cache)


def shards(n, nh, queries, cache, page_table, page_count, out_weight):
    me = lax.axis_index("seq")
    my_head = lax.axis_index("head")
    _, pages, kv, page_len, head_dim = cache.shape
    local, heads, _ = queries.shape
    group = heads // kv
    batch, slots = page_table.shape
    bits = [1 << i for i in range(n.bit_length() - 1)]
    outer = bits[1:]
    halves = 2
    half = local // halves
    orders = [outer, outer[1::-1] + outer[2:]]

    def swap(x, bit):
        return lax.ppermute(x, "seq", [(i, i ^ bit) for i in range(n)])

    per = half * n // 2
    rel = []
    for a in range(halves):
        for c in range(2):
            for s in range(n // 2):
                j = c * bits[0]
                for at, bit in enumerate(orders[a]):
                    if (s >> (len(outer) - 1 - at)) & 1:
                        j |= bit
                rel.append((j, a))
    rel_j = jnp.array([j for j, _ in rel], jnp.int32)
    rel_a = jnp.array([a for _, a in rel], jnp.int32)
    true_block = (rel_j ^ me) * halves + rel_a

    table = page_table.reshape(-1, half, slots)[true_block].reshape(batch, slots)
    counts = page_count.reshape(-1, half)[true_block].reshape(batch)

    got = [queries[a * half : (a + 1) * half] for a in range(halves)]
    lists = None
    for at in reversed(range(len(outer))):
        new = [swap(x, orders[a][at]) for a, x in enumerate(got)]
        if at == 0:
            lists = make_lists(me, table, counts, pages)
            new, lists = lax.optimization_barrier((new, lists))
        elif at == len(outer) - 1:
            new, table, counts = lax.optimization_barrier((new, table, counts))
        got = [jnp.concatenate([x, y], axis=0) for x, y in zip(got, new)]
    q_parts = []
    for x in got:
        q_parts += [x, swap(x, bits[0])]

    parts = attend(*lists, q_parts, cache)

    keep = [parts[2 * a] for a in range(halves)]
    send = [parts[2 * a + 1] for a in range(halves)]
    now = per
    att = [None] * halves
    for at in range(len(bits)):
        took = [swap(send[a], ([bits[0]] + orders[a])[at]) for a in range(halves)]
        for a in range(halves):
            last = at == len(bits) - 1
            res = merge(keep[a], took[a], now, heads, last)
            if last:
                att[a] = res[0].reshape(half, heads * head_dim)
            else:
                keep[a], send[a] = res
        now //= 2

    for at in reversed(range(len(outer))):
        new = [swap(x, orders[a][at]) for a, x in enumerate(att)]
        att = [jnp.concatenate([x, y], axis=0) for x, y in zip(att, new)]
    rows = []
    for x in att:
        rows += [x, swap(x, bits[0])]
    product = jnp.dot(jnp.concatenate(rows, axis=0), out_weight, preferred_element_type=jnp.float32)

    width = product.shape[1]
    place = {ja: i for i, ja in enumerate(rel)}
    inverse = jnp.array([place[(j, a)] for j in range(n) for a in range(halves)], jnp.int32).reshape(n, halves)
    source = inverse[jnp.arange(n, dtype=jnp.int32) ^ me].reshape(nh, -1)
    blocks = product.reshape(n * halves, half, width)
    out = blocks[source[my_head]].reshape(batch // nh, width)
    for step in range(1, nh):
        give = blocks[source[my_head ^ step]].astype(jnp.bfloat16).reshape(batch // nh, width)
        took = lax.ppermute(give, "head", [(i, i ^ step) for i in range(nh)])
        out = out + took.astype(jnp.float32)
    return out.astype(jnp.bfloat16)


def solution(mesh):
    n, nh = mesh.shape["seq"], mesh.shape["head"]
    return jax.shard_map(
        functools.partial(shards, n, nh),
        mesh=mesh,
        in_specs=(
            P("seq", "head", None),
            P(None, "seq", "head", None, None),
            P(),
            P(),
            P("head", "seq"),
        ),
        out_specs=P("head", "seq"),
        check_vma=False,
    )
```

```python
import functools
import math

import jax
import jax.numpy as jnp
from jax import lax
from jax.experimental import pallas as pl
from jax.experimental.pallas import tpu as pltpu
from jax.sharding import PartitionSpec as P

CAP = 4
TILE = 16
SEGMENTS = 4
TOGETHER = 4
UNROLL = 4
LEAD = 2 * TOGETHER
NONE = -1e30
PLANES = 3
LANES = 128


def call(body, out_shape, in_specs, out_specs, flops, moved, **kw):
    return pl.pallas_call(
        body,
        out_shape=out_shape,
        in_specs=in_specs,
        out_specs=out_specs,
        cost_estimate=pl.CostEstimate(flops=flops, bytes_accessed=moved, transcendentals=0),
        **kw,
    )


SMEM = pl.BlockSpec(memory_space=pltpu.SMEM)
VMEM = pl.BlockSpec(memory_space=pltpu.VMEM)
ANY = pl.BlockSpec(memory_space=pl.ANY)


def list_kernel(pages, me_ref, table_ref, count_ref, lst_ref, gp_ref, start_ref, valid_ref):
    batch, slots = table_ref.shape
    most = gp_ref.shape[1]
    f32, bf16, i32 = jnp.float32, jnp.bfloat16, jnp.int32

    def iota(shape, axis):
        return lax.broadcasted_iota(i32, shape, axis)

    def ones_where(mask):
        return jnp.where(mask, 1.0, 0.0).astype(bf16)

    def dot(x, y, dims=((1,), (0,)), **kw):
        return lax.dot_general(x, y, (dims, ((), ())), preferred_element_type=f32, **kw)

    page = table_ref[...] - me_ref[0] * pages
    present = (iota((batch, slots), 1) < count_ref[...]) & (page >= 0) & (page < pages)
    here = ones_where(present)
    upto = dot(here, ones_where(iota((slots, slots), 0) <= iota((slots, slots), 1)))
    valid_ref[...] = dot(jnp.ones((8, slots), bf16), here, ((1,), (1,)))[:1].astype(i32)
    hot = []
    for r in range(CAP):
        mine = present & (upto == r + 1.0)
        chosen = jnp.max(jnp.where(mine, page, -1), axis=1, keepdims=True)
        hot.append(jnp.where(iota((batch, pages), 1) == chosen, 1.0, 0.0))
    every = sum(hot[1:], hot[0]).astype(bf16)
    before = dot(ones_where(iota((batch, batch), 0) > iota((batch, batch), 1)), every)

    def groups(n):
        return jnp.floor((n + (TILE - 1.0)) * (1.0 / TILE))

    exact = dict(precision=lax.Precision.HIGHEST)
    row = groups(dot(jnp.ones((8, batch), bf16), every))
    under = jnp.where(iota((pages, pages), 0) < iota((pages, pages), 1), 1.0, 0.0)
    base = dot(row, under, **exact)[:1] + LEAD
    place = base * TILE + before
    col = groups(dot(every, jnp.ones((batch, LANES), bf16), ((0,), (0,))))
    over = jnp.where(iota((pages, pages), 1) < iota((pages, pages), 0), 1.0, 0.0)
    base_col = dot(over, col, **exact)[:, :1] + LEAD
    at_most = jnp.where(base_col <= iota((pages, most), 1).astype(f32), 1.0, 0.0)
    gp_ref[...] = jnp.maximum(jnp.sum(at_most, axis=0, keepdims=True) - 1.0, 0.0).astype(i32)

    bound = iota((pages, LANES), 1) * (pages // SEGMENTS)
    start_ref[...] = jnp.sum(jnp.where(iota((pages, LANES), 0) < bound, col, 0.0), axis=0, keepdims=True).astype(i32)

    size = lst_ref.shape[1]
    total = jnp.zeros((8, size), f32)
    for r in range(CAP):
        to = jnp.sum(jnp.where(hot[r] > 0.0, place + 1.0, 0.0), axis=1, keepdims=True).astype(i32) - 1
        onto = ones_where(iota((batch, size), 1) == to)
        pair = iota((8, batch), 1) * CAP + r
        which = iota((8, batch), 0)
        parts = jnp.where(which == 0, pair // 64, jnp.where(which == 1, pair % 64, 1)).astype(f32)
        total = total + dot(parts.astype(bf16), onto)
    found = total[0:1] * 64.0 + total[1:2]
    lst_ref[...] = jnp.where(total[2:3] > 0.5, found, float(batch * CAP)).astype(i32)


def make_lists(me, table, counts, pages):
    batch, slots = table.shape
    most = -(-(pages + batch * CAP // TILE + 2 * LEAD + TOGETHER) // 8) * 8
    shapes = [(1, most * TILE), (1, most), (1, LANES), (1, batch)]
    return call(
        functools.partial(list_kernel, pages),
        [jax.ShapeDtypeStruct(s, jnp.int32) for s in shapes],
        [SMEM, VMEM, VMEM],
        [VMEM] * 4,
        10**8,
        10**6,
        name="lists",
        compiler_params=pltpu.CompilerParams(vmem_limit_bytes=16 * 2**20),
    )(me.reshape(1), table, counts.reshape(batch, 1))


def stat_rows(count, heads):
    return heads if PLANES * count <= LANES else PLANES * heads


def split3(x, count):
    parts = []
    for _ in range(PLANES):
        part = x.astype(jnp.bfloat16).astype(jnp.float32)
        parts.append(part)
        x = x - part
    if PLANES * count > LANES:
        x = jnp.concatenate(parts, axis=0)
        if x.shape[1] < LANES:
            x = jnp.concatenate([x, jnp.zeros((x.shape[0], LANES - x.shape[1]), jnp.float32)], axis=1)
        return x.astype(jnp.bfloat16)
    parts = [p[:, :count] for p in parts]
    rest = LANES - PLANES * count
    if rest:
        parts.append(jnp.zeros((x.shape[0], rest), jnp.float32))
    return jnp.concatenate(parts, axis=1).astype(jnp.bfloat16)


def join3(block, count, heads):
    x = block.astype(jnp.float32)
    if PLANES * count > LANES:
        parts = [x[p * heads : (p + 1) * heads, :count] for p in range(PLANES)]
    else:
        parts = [x[:, p * count : (p + 1) * count] for p in range(PLANES)]
    return (parts[0] + parts[1]) + parts[2]


def attention_kernel(nq, kv, group, scale, lst, gp, start, valid, *refs):
    q_refs = refs[:nq]
    cache = refs[nq]
    outs = refs[nq + 1 : 2 * nq + 1]
    kbuf, vbuf, sems, q32, osc, lsc, ssc, msc, psc = refs[2 * nq + 1 :]
    per = q_refs[0].shape[0]
    heads = kv * group
    pairs = nq * per * CAP
    head_dim = vbuf.shape[-1]
    chunk = kbuf.shape[0] // SEGMENTS
    ones = jnp.ones(vbuf.shape[-2:-1] + (LANES,), jnp.bfloat16)

    def copies(g):
        at = pl.ds(g * chunk, chunk)
        return (
            pltpu.make_async_copy(cache.at[0, at], kbuf.at[at], sems.at[0, g]),
            pltpu.make_async_copy(cache.at[1, at], vbuf.at[at], sems.at[1, g]),
        )

    for c in copies(0):
        c.start()

    def convert(a, i):
        for u in range(8):
            row = q_refs[a][i * 8 + u].astype(jnp.float32)
            q32[a * per + i * 8 + u] = row.reshape(kv, group, head_dim)

    for a in range(nq):
        pl.loop(0, per // 8)(functools.partial(convert, a))
    q32[nq * per] = jnp.zeros((kv, group, head_dim), jnp.float32)
    osc[pairs + 1] = jnp.zeros((heads, head_dim), jnp.bfloat16)
    lsc[pairs + 1] = jnp.full((kv, group, LANES), NONE, jnp.float32)

    def step(j):
        def entries(stage, v):
            i = (j + stage) * TOGETHER + v
            return gp[0, i], [lst[0, i * TILE + u] for u in range(TILE)]

        for v in range(TOGETHER):
            page, t = entries(0, v)
            os = []
            for k in range(kv):
                values = jnp.concatenate([vbuf[page, k], ones], axis=1)
                o = jnp.dot(psc[v, k], values, preferred_element_type=jnp.float32)
                total = o[:, head_dim:]
                os.append(o[:, :head_dim] * (1.0 / total))
                lse = msc[v, k] + jnp.log2(total)
                for u in range(TILE):
                    lsc[t[u], k] = lse[u * group : (u + 1) * group]
            for u in range(TILE):
                tiles = [o[u * group : (u + 1) * group] for o in os]
                osc[t[u]] = jnp.concatenate(tiles, axis=0).astype(jnp.bfloat16)
        for v in range(TOGETHER):
            for k in range(kv):
                s = ssc[v, k]
                m = jnp.broadcast_to(jnp.max(s, axis=1, keepdims=True), s.shape)
                psc[v, k] = jnp.exp2(s - m).astype(jnp.bfloat16)
                msc[v, k] = m
        for v in range(TOGETHER):
            page, t = entries(2, v)
            b = [x // CAP for x in t]
            for k in range(kv):
                rows = jnp.concatenate([q32[x, k] for x in b], axis=0)
                s = lax.dot_general(
                    rows.astype(jnp.bfloat16),
                    kbuf[page, k],
                    (((1,), (1,)), ((), ())),
                    preferred_element_type=jnp.float32,
                )
                ssc[v, k] = s * scale

    for g in range(SEGMENTS):
        for c in copies(g):
            c.wait()
        if g + 1 < SEGMENTS:
            for c in copies(g + 1):
                c.start()
        end = start[0, g + 1]
        if g == SEGMENTS - 1:
            end = end + (3 * TOGETHER - 1)
        pl.loop(start[0, g] // TOGETHER, end // TOGETHER)(step)

    lane = lax.broadcasted_iota(jnp.int32, (heads, LANES), 1)
    for a in range(nq):

        def finish(s, stats):
            b = a * per + s
            n = valid[0, b]
            t = [jnp.where(n > r, b * CAP + r, pairs + 1) for r in range(CAP)]
            l = [lsc[x].reshape(heads, LANES) for x in t]
            top = functools.reduce(jnp.maximum, l)
            w = [jnp.exp2(x - top) for x in l]
            total = sum(w[1:], w[0])
            terms = [x * osc[y].astype(jnp.float32) for x, y in zip(w, t)]
            o = sum(terms[1:], terms[0]) * (1.0 / total)
            outs[a][pl.ds(pl.multiple_of(s * heads, heads), heads), :] = o.astype(jnp.bfloat16)
            return jnp.where(lane == s, top + jnp.log2(total), stats)

        stats = lax.fori_loop(0, per, finish, jnp.full((heads, LANES), NONE, jnp.float32), unroll=UNROLL)
        outs[a][per * heads :, :] = split3(stats, per)


def merge_kernel(per, heads, last, keep, recv, *outs):
    rows = per * heads
    half = per // 2
    la = join3(keep[rows:, :], per, heads)
    lb = join3(recv[rows:, :], per, heads)
    if last:
        lb = jnp.concatenate([lb[:, half:], lb[:, :half]], axis=1)
    diff = la - lb
    weight = 1.0 / (1.0 + jnp.exp2(-diff))
    each = per // len(outs)
    for s in range(per):
        other = (s + half) % per if last else s
        x = keep[s * heads : (s + 1) * heads, :].astype(jnp.float32)
        y = recv[other * heads : (other + 1) * heads, :].astype(jnp.float32)
        z = y + weight[:, s : s + 1] * (x - y)
        at = s % each
        outs[s // each][at * heads : (at + 1) * heads, :] = z.astype(jnp.bfloat16)
    if not last:
        stats = jnp.maximum(la, lb) + jnp.log2(1.0 + jnp.exp2(-jnp.abs(diff)))
        for i, out in enumerate(outs):
            out[each * heads :, :] = split3(stats[:, i * each : (i + 1) * each], each)


def merge(keep, recv, per, heads, pieces, last):
    each = per // pieces
    rows = each * heads + (0 if last else stat_rows(each, heads))
    return call(
        functools.partial(merge_kernel, per, heads, last),
        [jax.ShapeDtypeStruct((rows, LANES), jnp.bfloat16)] * pieces,
        [VMEM] * 2,
        [VMEM] * pieces,
        keep.size * 8,
        keep.size * 6,
        name="merge",
        compiler_params=pltpu.CompilerParams(vmem_limit_bytes=8 * 2**20),
    )(keep, recv)


def attend(lst, gp, start, valid, q_parts, cache):
    nq = len(q_parts)
    per, heads, head_dim = q_parts[0].shape
    _, pages, kv, page_len, _ = cache.shape
    group = heads // kv
    batch = nq * per
    pairs = batch * CAP
    scratch = [pltpu.VMEM(cache.shape[1:], cache.dtype)] * 2 + [pltpu.SemaphoreType.DMA((2, SEGMENTS))]
    scratch += [pltpu.VMEM((batch + 1, kv, group, head_dim), jnp.float32)]
    scratch += [pltpu.VMEM((pairs + 2, heads, head_dim), jnp.bfloat16)]
    scratch += [pltpu.VMEM((pairs + 2, kv, group, LANES), jnp.float32)]
    scratch += [pltpu.VMEM((TOGETHER, kv, TILE * group, page_len), jnp.float32)] * 2
    scratch += [pltpu.VMEM((TOGETHER, kv, TILE * group, page_len), jnp.bfloat16)]
    return call(
        functools.partial(attention_kernel, nq, kv, group, math.log2(math.e) / math.sqrt(head_dim)),
        [jax.ShapeDtypeStruct((per * heads + stat_rows(per, heads), LANES), jnp.bfloat16)] * nq,
        [SMEM] * 4 + [VMEM] * nq + [ANY],
        [VMEM] * nq,
        4 * pairs * heads * page_len * head_dim,
        cache.size * 2,
        scratch_shapes=scratch,
        name="attention",
        compiler_params=pltpu.CompilerParams(vmem_limit_bytes=47 * 2**20),
    )(lst, gp, start, valid, *q_parts, cache)


def shards(n, nh, queries, cache, page_table, page_count, out_weight):
    me = lax.axis_index("seq")
    my_head = lax.axis_index("head")
    _, pages, kv, page_len, head_dim = cache.shape
    local, heads, _ = queries.shape
    group = heads // kv
    batch, slots = page_table.shape
    bits = [1 << i for i in range(n.bit_length() - 1)]
    outer = bits[1:]
    halves = 2
    half = local // halves
    orders = [outer, outer[1::-1] + outer[2:]]

    def swap(x, bit):
        return lax.ppermute(x, "seq", [(i, i ^ bit) for i in range(n)])

    per = half * n // 2
    rel = []
    for a in range(halves):
        for c in range(2):
            for s in range(n // 2):
                j = c * bits[0]
                for at, bit in enumerate(orders[a]):
                    if (s >> (len(outer) - 1 - at)) & 1:
                        j |= bit
                rel.append((j, a))
    rel_j = jnp.array([j for j, _ in rel], jnp.int32)
    rel_a = jnp.array([a for _, a in rel], jnp.int32)
    true_block = (rel_j ^ me) * halves + rel_a

    table = page_table.reshape(-1, half, slots)[true_block].reshape(batch, slots)
    counts = page_count.reshape(-1, half)[true_block].reshape(batch)

    got = [queries[a * half : (a + 1) * half] for a in range(halves)]
    lists = None
    for at in reversed(range(len(outer))):
        new = [swap(x, orders[a][at]) for a, x in enumerate(got)]
        if at == 0:
            lists = make_lists(me, table, counts, pages)
            new, lists = lax.optimization_barrier((new, lists))
        elif at == len(outer) - 1:
            new, table, counts = lax.optimization_barrier((new, table, counts))
        got = [jnp.concatenate([x, y], axis=0) for x, y in zip(got, new)]
    q_parts = []
    for x in got:
        q_parts += [x, swap(x, bits[0])]

    parts = attend(*lists, q_parts, cache)

    keep = [parts[2 * a] for a in range(halves)]
    send = [parts[2 * a + 1] for a in range(halves)]
    now = per
    for at in range(len(bits)):
        last = at == len(bits) - 1
        took = [swap(send[a], ([bits[0]] + orders[a])[at]) for a in range(halves)]
        pieces = 2 if at < len(bits) - 2 else 1
        for a in range(halves):
            res = merge(keep[a], took[a], now, heads, pieces, last)
            keep[a], send[a] = res[0], res[-1]
        now //= pieces
    att = [x.reshape(now, heads * head_dim) for x in keep]

    for at in reversed(range(len(outer) - 1)):
        new = [swap(x, orders[a][at]) for a, x in enumerate(att)]
        att = [jnp.concatenate([x, y], axis=0) for x, y in zip(att, new)]
    others = [swap(x, bits[0]) for x in att]
    product = jnp.concatenate(
        [
            jnp.dot(jnp.concatenate(x, axis=0), out_weight, preferred_element_type=jnp.float32)
            for x in (att, others)
        ],
        axis=0,
    )

    width = product.shape[1]
    place = {(j, a): ((j & 1) * halves + a) * (n // 2) + i % (n // 2) for i, (j, a) in enumerate(rel)}
    inverse = jnp.array([place[(j, a)] for j in range(n) for a in range(halves)], jnp.int32).reshape(n, halves)
    source = inverse[jnp.arange(n, dtype=jnp.int32) ^ me].reshape(nh, -1)
    blocks = product.reshape(n * halves, half, width)
    out = blocks[source[my_head]].reshape(batch // nh, width)
    for step in range(1, nh):
        give = blocks[source[my_head ^ step]].astype(jnp.bfloat16).reshape(batch // nh, width)
        took = lax.ppermute(give, "head", [(i, i ^ step) for i in range(nh)])
        out = out + took.astype(jnp.float32)
    return out.astype(jnp.bfloat16)


def solution(mesh):
    n, nh = mesh.shape["seq"], mesh.shape["head"]
    return jax.shard_map(
        functools.partial(shards, n, nh),
        mesh=mesh,
        in_specs=(
            P("seq", "head", None),
            P(None, "seq", "head", None, None),
            P(),
            P(),
            P("head", "seq"),
        ),
        out_specs=P("head", "seq"),
        check_vma=False,
    )
```

```python
import functools
import math

import jax
import jax.numpy as jnp
from jax import lax
from jax.experimental import pallas as pl
from jax.experimental.pallas import tpu as pltpu
from jax.sharding import PartitionSpec as P

CAP = 4
TILE = 16
SEGMENTS = 4
TOGETHER = 4
UNROLL = 8
LEAD = 2 * TOGETHER
NONE = -1e30
PLANES = 3
LANES = 128


def call(body, out_shape, in_specs, out_specs, flops, moved, **kw):
    return pl.pallas_call(
        body,
        out_shape=out_shape,
        in_specs=in_specs,
        out_specs=out_specs,
        cost_estimate=pl.CostEstimate(flops=flops, bytes_accessed=moved, transcendentals=0),
        **kw,
    )


SMEM = pl.BlockSpec(memory_space=pltpu.SMEM)
VMEM = pl.BlockSpec(memory_space=pltpu.VMEM)
ANY = pl.BlockSpec(memory_space=pl.ANY)


def list_kernel(pages, me_ref, table_ref, count_ref, lst_ref, gp_ref, start_ref, valid_ref):
    batch, slots = table_ref.shape
    most = gp_ref.shape[1]
    f32, bf16, i32 = jnp.float32, jnp.bfloat16, jnp.int32

    def iota(shape, axis):
        return lax.broadcasted_iota(i32, shape, axis)

    def ones_where(mask):
        return jnp.where(mask, 1.0, 0.0).astype(bf16)

    def dot(x, y, dims=((1,), (0,)), **kw):
        return lax.dot_general(x, y, (dims, ((), ())), preferred_element_type=f32, **kw)

    page = table_ref[...] - me_ref[0] * pages
    present = (iota((batch, slots), 1) < count_ref[...]) & (page >= 0) & (page < pages)
    here = ones_where(present)
    upto = dot(here, ones_where(iota((slots, slots), 0) <= iota((slots, slots), 1)))
    valid_ref[...] = dot(jnp.ones((8, slots), bf16), here, ((1,), (1,)))[:1].astype(i32)
    hot = []
    for r in range(CAP):
        mine = present & (upto == r + 1.0)
        chosen = jnp.max(jnp.where(mine, page, -1), axis=1, keepdims=True)
        hot.append(jnp.where(iota((batch, pages), 1) == chosen, 1.0, 0.0))
    every = sum(hot[1:], hot[0]).astype(bf16)
    before = dot(ones_where(iota((batch, batch), 0) > iota((batch, batch), 1)), every)

    def groups(n):
        return jnp.floor((n + (TILE - 1.0)) * (1.0 / TILE))

    exact = dict(precision=lax.Precision.HIGHEST)
    row = groups(dot(jnp.ones((8, batch), bf16), every))
    under = jnp.where(iota((pages, pages), 0) < iota((pages, pages), 1), 1.0, 0.0)
    base = dot(row, under, **exact)[:1] + LEAD
    place = base * TILE + before
    col = groups(dot(every, jnp.ones((batch, LANES), bf16), ((0,), (0,))))
    over = jnp.where(iota((pages, pages), 1) < iota((pages, pages), 0), 1.0, 0.0)
    base_col = dot(over, col, **exact)[:, :1] + LEAD
    at_most = jnp.where(base_col <= iota((pages, most), 1).astype(f32), 1.0, 0.0)
    gp_ref[...] = jnp.maximum(jnp.sum(at_most, axis=0, keepdims=True) - 1.0, 0.0).astype(i32)

    bound = iota((pages, LANES), 1) * (pages // SEGMENTS)
    start_ref[...] = jnp.sum(jnp.where(iota((pages, LANES), 0) < bound, col, 0.0), axis=0, keepdims=True).astype(i32)

    size = lst_ref.shape[1]
    total = jnp.zeros((8, size), f32)
    for r in range(CAP):
        to = jnp.sum(jnp.where(hot[r] > 0.0, place + 1.0, 0.0), axis=1, keepdims=True).astype(i32) - 1
        onto = ones_where(iota((batch, size), 1) == to)
        pair = iota((8, batch), 1) * CAP + r
        which = iota((8, batch), 0)
        parts = jnp.where(which == 0, pair // 64, jnp.where(which == 1, pair % 64, 1)).astype(f32)
        total = total + dot(parts.astype(bf16), onto)
    found = total[0:1] * 64.0 + total[1:2]
    lst_ref[...] = jnp.where(total[2:3] > 0.5, found, float(batch * CAP)).astype(i32)


def make_lists(me, table, counts, pages):
    batch, slots = table.shape
    most = -(-(pages + batch * CAP // TILE + 2 * LEAD + TOGETHER) // 8) * 8
    shapes = [(1, most * TILE), (1, most), (1, LANES), (1, batch)]
    return call(
        functools.partial(list_kernel, pages),
        [jax.ShapeDtypeStruct(s, jnp.int32) for s in shapes],
        [SMEM, VMEM, VMEM],
        [VMEM] * 4,
        10**8,
        10**6,
        name="lists",
        compiler_params=pltpu.CompilerParams(vmem_limit_bytes=16 * 2**20),
    )(me.reshape(1), table, counts.reshape(batch, 1))


def stat_rows(count, heads):
    return heads if PLANES * count <= LANES else PLANES * heads


def split3(x, count):
    parts = []
    for _ in range(PLANES):
        part = x.astype(jnp.bfloat16).astype(jnp.float32)
        parts.append(part)
        x = x - part
    if PLANES * count > LANES:
        x = jnp.concatenate(parts, axis=0)
        if x.shape[1] < LANES:
            x = jnp.concatenate([x, jnp.zeros((x.shape[0], LANES - x.shape[1]), jnp.float32)], axis=1)
        return x.astype(jnp.bfloat16)
    parts = [p[:, :count] for p in parts]
    rest = LANES - PLANES * count
    if rest:
        parts.append(jnp.zeros((x.shape[0], rest), jnp.float32))
    return jnp.concatenate(parts, axis=1).astype(jnp.bfloat16)


def join3(block, count, heads):
    x = block.astype(jnp.float32)
    if PLANES * count > LANES:
        parts = [x[p * heads : (p + 1) * heads, :count] for p in range(PLANES)]
    else:
        parts = [x[:, p * count : (p + 1) * count] for p in range(PLANES)]
    return (parts[0] + parts[1]) + parts[2]


def attention_kernel(nq, kv, group, scale, lst, gp, start, valid, *refs):
    q_refs = refs[:nq]
    cache = refs[nq]
    outs = refs[nq + 1 : 2 * nq + 1]
    kbuf, vbuf, sems, q32, osc, lsc, ssc, msc, psc = refs[2 * nq + 1 :]
    per = q_refs[0].shape[0]
    heads = kv * group
    pairs = nq * per * CAP
    head_dim = vbuf.shape[-1]
    chunk = kbuf.shape[0] // SEGMENTS
    ones = jnp.ones(vbuf.shape[-2:-1] + (LANES,), jnp.bfloat16)

    def copies(g):
        at = pl.ds(g * chunk, chunk)
        return (
            pltpu.make_async_copy(cache.at[0, at], kbuf.at[at], sems.at[0, g]),
            pltpu.make_async_copy(cache.at[1, at], vbuf.at[at], sems.at[1, g]),
        )

    for c in copies(0):
        c.start()

    def convert(a, i):
        for u in range(8):
            row = q_refs[a][i * 8 + u].astype(jnp.float32)
            q32[a * per + i * 8 + u] = row.reshape(kv, group, head_dim)

    for a in range(nq):
        pl.loop(0, per // 8)(functools.partial(convert, a))
    q32[nq * per] = jnp.zeros((kv, group, head_dim), jnp.float32)
    osc[pairs + 1] = jnp.zeros((heads, head_dim), jnp.bfloat16)
    lsc[pairs + 1] = jnp.full((kv, group, LANES), NONE, jnp.float32)

    def step(j):
        def entries(stage, v):
            i = (j + stage) * TOGETHER + v
            return gp[0, i], [lst[0, i * TILE + u] for u in range(TILE)]

        for v in range(TOGETHER):
            page, t = entries(0, v)
            os = []
            for k in range(kv):
                values = jnp.concatenate([vbuf[page, k], ones], axis=1)
                o = jnp.dot(psc[v, k], values, preferred_element_type=jnp.float32)
                total = o[:, head_dim:]
                os.append(o[:, :head_dim] * (1.0 / total))
                lse = msc[v, k] + jnp.log2(total)
                for u in range(TILE):
                    lsc[t[u], k] = lse[u * group : (u + 1) * group]
            for u in range(TILE):
                tiles = [o[u * group : (u + 1) * group] for o in os]
                osc[t[u]] = jnp.concatenate(tiles, axis=0).astype(jnp.bfloat16)
        for v in range(TOGETHER):
            for k in range(kv):
                s = ssc[v, k]
                m = jnp.broadcast_to(jnp.max(s, axis=1, keepdims=True), s.shape)
                psc[v, k] = jnp.exp2(s - m).astype(jnp.bfloat16)
                msc[v, k] = m
        for v in range(TOGETHER):
            page, t = entries(2, v)
            b = [x // CAP for x in t]
            for k in range(kv):
                rows = jnp.concatenate([q32[x, k] for x in b], axis=0)
                s = lax.dot_general(
                    rows.astype(jnp.bfloat16),
                    kbuf[page, k],
                    (((1,), (1,)), ((), ())),
                    preferred_element_type=jnp.float32,
                )
                ssc[v, k] = s * scale

    for g in range(SEGMENTS):
        for c in copies(g):
            c.wait()
        if g + 1 < SEGMENTS:
            for c in copies(g + 1):
                c.start()
        end = start[0, g + 1]
        if g == SEGMENTS - 1:
            end = end + (3 * TOGETHER - 1)
        pl.loop(start[0, g] // TOGETHER, end // TOGETHER)(step)

    lane = lax.broadcasted_iota(jnp.int32, (heads, LANES), 1)
    for a in range(nq):

        def finish(s, stats):
            b = a * per + s
            n = valid[0, b]
            t = [jnp.where(n > r, b * CAP + r, pairs + 1) for r in range(CAP)]
            l = [lsc[x].reshape(heads, LANES) for x in t]
            top = functools.reduce(jnp.maximum, l)
            w = [jnp.exp2(x - top) for x in l]
            total = sum(w[1:], w[0])
            terms = [x * osc[y].astype(jnp.float32) for x, y in zip(w, t)]
            o = sum(terms[1:], terms[0]) * (1.0 / total)
            outs[a][pl.ds(pl.multiple_of(s * heads, heads), heads), :] = o.astype(jnp.bfloat16)
            return jnp.where(lane == s, top + jnp.log2(total), stats)

        stats = lax.fori_loop(0, per, finish, jnp.full((heads, LANES), NONE, jnp.float32), unroll=UNROLL)
        outs[a][per * heads :, :] = split3(stats, per)


def merge_kernel(per, heads, last, keep, recv, *outs):
    rows = per * heads
    half = per // 2
    la = join3(keep[rows:, :], per, heads)
    lb = join3(recv[rows:, :], per, heads)
    if last:
        lb = jnp.concatenate([lb[:, half:], lb[:, :half]], axis=1)
    diff = la - lb
    weight = 1.0 / (1.0 + jnp.exp2(-diff))
    each = per // len(outs)
    for s in range(per):
        other = (s + half) % per if last else s
        x = keep[s * heads : (s + 1) * heads, :].astype(jnp.float32)
        y = recv[other * heads : (other + 1) * heads, :].astype(jnp.float32)
        z = y + weight[:, s : s + 1] * (x - y)
        at = s % each
        outs[s // each][at * heads : (at + 1) * heads, :] = z.astype(jnp.bfloat16)
    if not last:
        stats = jnp.maximum(la, lb) + jnp.log2(1.0 + jnp.exp2(-jnp.abs(diff)))
        for i, out in enumerate(outs):
            out[each * heads :, :] = split3(stats[:, i * each : (i + 1) * each], each)


def merge(keep, recv, per, heads, pieces, last):
    each = per // pieces
    rows = each * heads + (0 if last else stat_rows(each, heads))
    return call(
        functools.partial(merge_kernel, per, heads, last),
        [jax.ShapeDtypeStruct((rows, LANES), jnp.bfloat16)] * pieces,
        [VMEM] * 2,
        [VMEM] * pieces,
        keep.size * 8,
        keep.size * 6,
        name="merge",
        compiler_params=pltpu.CompilerParams(vmem_limit_bytes=8 * 2**20),
    )(keep, recv)


def attend(lst, gp, start, valid, q_parts, cache):
    nq = len(q_parts)
    per, heads, head_dim = q_parts[0].shape
    _, pages, kv, page_len, _ = cache.shape
    group = heads // kv
    batch = nq * per
    pairs = batch * CAP
    scratch = [pltpu.VMEM(cache.shape[1:], cache.dtype)] * 2 + [pltpu.SemaphoreType.DMA((2, SEGMENTS))]
    scratch += [pltpu.VMEM((batch + 1, kv, group, head_dim), jnp.float32)]
    scratch += [pltpu.VMEM((pairs + 2, heads, head_dim), jnp.bfloat16)]
    scratch += [pltpu.VMEM((pairs + 2, kv, group, LANES), jnp.float32)]
    scratch += [pltpu.VMEM((TOGETHER, kv, TILE * group, page_len), jnp.float32)] * 2
    scratch += [pltpu.VMEM((TOGETHER, kv, TILE * group, page_len), jnp.bfloat16)]
    return call(
        functools.partial(attention_kernel, nq, kv, group, math.log2(math.e) / math.sqrt(head_dim)),
        [jax.ShapeDtypeStruct((per * heads + stat_rows(per, heads), LANES), jnp.bfloat16)] * nq,
        [SMEM] * 4 + [VMEM] * nq + [ANY],
        [VMEM] * nq,
        4 * pairs * heads * page_len * head_dim,
        cache.size * 2,
        scratch_shapes=scratch,
        name="attention",
        compiler_params=pltpu.CompilerParams(vmem_limit_bytes=47 * 2**20),
    )(lst, gp, start, valid, *q_parts, cache)


def shards(n, nh, queries, cache, page_table, page_count, out_weight):
    me = lax.axis_index("seq")
    my_head = lax.axis_index("head")
    _, pages, kv, page_len, head_dim = cache.shape
    local, heads, _ = queries.shape
    group = heads // kv
    batch, slots = page_table.shape
    bits = [1 << i for i in range(n.bit_length() - 1)]
    outer = bits[1:]
    halves = 2
    half = local // halves
    orders = [outer, outer[1::-1] + outer[2:]]

    def swap(x, bit):
        return lax.ppermute(x, "seq", [(i, i ^ bit) for i in range(n)])

    per = half * n // 2
    rel = []
    for a in range(halves):
        for c in range(2):
            for s in range(n // 2):
                j = c * bits[0]
                for at, bit in enumerate(orders[a]):
                    if (s >> (len(outer) - 1 - at)) & 1:
                        j |= bit
                rel.append((j, a))
    rel_j = jnp.array([j for j, _ in rel], jnp.int32)
    rel_a = jnp.array([a for _, a in rel], jnp.int32)
    true_block = (rel_j ^ me) * halves + rel_a

    table = page_table.reshape(-1, half, slots)[true_block].reshape(batch, slots)
    counts = page_count.reshape(-1, half)[true_block].reshape(batch)

    got = [queries[a * half : (a + 1) * half] for a in range(halves)]
    lists = None
    for at in reversed(range(len(outer))):
        new = [swap(x, orders[a][at]) for a, x in enumerate(got)]
        if at == 0:
            lists = make_lists(me, table, counts, pages)
            new, lists = lax.optimization_barrier((new, lists))
        elif at == len(outer) - 1:
            new, table, counts = lax.optimization_barrier((new, table, counts))
        got = [jnp.concatenate([x, y], axis=0) for x, y in zip(got, new)]
    q_parts = []
    for x in got:
        q_parts += [x, swap(x, bits[0])]

    parts = attend(*lists, q_parts, cache)

    keep = [parts[2 * a] for a in range(halves)]
    send = [parts[2 * a + 1] for a in range(halves)]
    now = per
    for at in range(len(bits)):
        last = at == len(bits) - 1
        took = [swap(send[a], ([bits[0]] + orders[a])[at]) for a in range(halves)]
        pieces = 2 if at < len(bits) - 2 else 1
        for a in range(halves):
            res = merge(keep[a], took[a], now, heads, pieces, last)
            keep[a], send[a] = res[0], res[-1]
        now //= pieces
    att = [x.reshape(now, heads * head_dim) for x in keep]

    for at in reversed(range(len(outer) - 1)):
        new = [swap(x, orders[a][at]) for a, x in enumerate(att)]
        att = [jnp.concatenate([x, y], axis=0) for x, y in zip(att, new)]
    others = [swap(x, bits[0]) for x in att]
    product = jnp.concatenate(
        [
            jnp.dot(jnp.concatenate(x, axis=0), out_weight, preferred_element_type=jnp.float32)
            for x in (att, others)
        ],
        axis=0,
    )

    width = product.shape[1]
    place = {(j, a): ((j & 1) * halves + a) * (n // 2) + i % (n // 2) for i, (j, a) in enumerate(rel)}
    inverse = jnp.array([place[(j, a)] for j in range(n) for a in range(halves)], jnp.int32).reshape(n, halves)
    source = inverse[jnp.arange(n, dtype=jnp.int32) ^ me].reshape(nh, -1)
    blocks = product.reshape(n * halves, half, width)
    out = blocks[source[my_head]].reshape(batch // nh, width)
    for step in range(1, nh):
        give = blocks[source[my_head ^ step]].astype(jnp.bfloat16).reshape(batch // nh, width)
        took = lax.ppermute(give, "head", [(i, i ^ step) for i in range(nh)])
        out = out + took.astype(jnp.float32)
    return out.astype(jnp.bfloat16)


def solution(mesh):
    n, nh = mesh.shape["seq"], mesh.shape["head"]
    return jax.shard_map(
        functools.partial(shards, n, nh),
        mesh=mesh,
        in_specs=(
            P("seq", "head", None),
            P(None, "seq", "head", None, None),
            P(),
            P(),
            P("head", "seq"),
        ),
        out_specs=P("head", "seq"),
        check_vma=False,
    )
```
